8 devices in a mesh: data: 8 (over z, y, x, core).
Axes of the slice: x: 2, y: 2, z: 1, core: 2. Of those that a mesh axis runs over, the one named last changes fastest.
Arguments:
- x_act: bfloat16 [128, 196, 384], P('data')
- y_tgt: bfloat16 [128, 196, 384], P('data')
- w_in: float32 [12, 384, 1536], replicated
- w_out: float32 [12, 1536, 384], replicated
Outputs:
- output 1: float32 [12, 384, 1536], replicated
- output 2: float32 [12, 1536, 384], replicated
- output 3: float32 [], replicated
All inputs are finite; a program needn't handle non-finite values.
Results may differ from the reference program's by a relative error of at most 0.00259924.
Values are sent between devices in bfloat16 or wider.
A program may use at most 1 GiB of HBM per device.

```python
import math
import jax
import jax.numpy as jnp
from jax import lax

D = 384
FF = 1536
SEQ = 196
LAYERS = 12
BATCH_DEV = 8
DEVICES = 8
MICRO_STEPS = 2
BLOCKS = DEVICES * MICRO_STEPS
BATCH_ALL = BLOCKS * BATCH_DEV
BLOCK_ROWS = BATCH_DEV * SEQ
RHO_RADIUS = 0.1 * math.sqrt(LAYERS * (D + FF))
LEARN_RATE = 1.0
TOK_SCALE = 1.0 / (BATCH_ALL * SEQ * D)


def setup_inputs(seed: int = 0) -> dict:
    root_key = jax.random.key(seed)
    k_x, k_y, k_in, k_out, k_gain = jax.random.split(root_key, 5)
    x_act = jax.random.normal(k_x, (BATCH_ALL, SEQ, D), jnp.float32).astype(jnp.bfloat16)
    y_tgt = jax.random.normal(k_y, (BATCH_ALL, SEQ, D), jnp.float32).astype(jnp.bfloat16)
    w_in = jax.random.normal(k_in, (LAYERS, D, FF), jnp.float32) * (D ** -0.5)
    layer_gain = jax.random.uniform(k_gain, (LAYERS, 1, 1), jnp.float32, 0.3, 0.9)
    w_out = jax.random.normal(k_out, (LAYERS, FF, D), jnp.float32) * (FF ** -0.5) * layer_gain
    return {"x_act": x_act, "y_tgt": y_tgt, "w_in": w_in, "w_out": w_out}


def gelu_tanh(z_val):
    return jax.nn.gelu(z_val, approximate=True)


def forward_layer(h_act, wi_cast, wo_cast):
    z_pre = jnp.dot(h_act, wi_cast, preferred_element_type=jnp.float32).astype(jnp.bfloat16)
    gelu_out = gelu_tanh(z_pre.astype(jnp.float32)).astype(jnp.bfloat16)
    u_out = jnp.dot(gelu_out, wo_cast, preferred_element_type=jnp.float32)
    return (h_act.astype(jnp.float32) + u_out).astype(jnp.bfloat16), z_pre


def block_sums(x_blk, y_blk, wi_cast, wo_cast):
    h_list = [x_blk]
    z_list = []
    for layer_idx in range(LAYERS):
        h_next, z_pre = forward_layer(h_list[-1], wi_cast[layer_idx], wo_cast[layer_idx])
        h_list.append(h_next)
        z_list.append(z_pre)
    out_err = h_list[-1].astype(jnp.float32) - y_blk.astype(jnp.float32)
    sq_sum = jnp.sum(out_err * out_err)
    back_grad = out_err.astype(jnp.bfloat16)
    sums_in = [None] * LAYERS
    sums_out = [None] * LAYERS
    for layer_idx in range(LAYERS - 1, -1, -1):
        gelu_out, gelu_vjp = jax.vjp(gelu_tanh, z_list[layer_idx].astype(jnp.float32))
        sums_out[layer_idx] = jnp.dot(gelu_out.astype(jnp.bfloat16).T, back_grad, preferred_element_type=jnp.float32)
        d_act = jnp.dot(back_grad, wo_cast[layer_idx].T, preferred_element_type=jnp.float32)
        d_pre = gelu_vjp(d_act)[0].astype(jnp.bfloat16)
        sums_in[layer_idx] = jnp.dot(h_list[layer_idx].T, d_pre, preferred_element_type=jnp.float32)
        if layer_idx > 0:
            back_in = jnp.dot(d_pre, wi_cast[layer_idx].T, preferred_element_type=jnp.float32)
            back_grad = (back_grad.astype(jnp.float32) + back_in).astype(jnp.bfloat16)
    return jnp.stack(sums_in), jnp.stack(sums_out), sq_sum


def grad_sums(x_blocks, y_blocks, wi_cast, wo_cast):
    def scan_body(acc_state, block_pair):
        acc_in, acc_out, acc_sq = acc_state
        s_in, s_out, s_sq = block_sums(block_pair[0], block_pair[1], wi_cast, wo_cast)
        return (acc_in + s_in, acc_out + s_out, acc_sq + s_sq), None
    init_state = (jnp.zeros((LAYERS, D, FF), jnp.float32), jnp.zeros((LAYERS, FF, D), jnp.float32), jnp.zeros((), jnp.float32))
    final_state, _ = lax.scan(scan_body, init_state, (x_blocks, y_blocks))
    return final_state


def reference(x_act, y_tgt, w_in, w_out):
    x_blocks = x_act.reshape(BLOCKS, BLOCK_ROWS, D)
    y_blocks = y_tgt.reshape(BLOCKS, BLOCK_ROWS, D)
    sum_in, sum_out, _ = grad_sums(x_blocks, y_blocks, w_in.astype(jnp.bfloat16), w_out.astype(jnp.bfloat16))
    grad_in = sum_in * TOK_SCALE
    grad_out = sum_out * TOK_SCALE
    grad_norm = jnp.sqrt(jnp.sum(grad_in * grad_in) + jnp.sum(grad_out * grad_out))
    perturb_coef = RHO_RADIUS / grad_norm
    pert_in = (w_in + perturb_coef * grad_in).astype(jnp.bfloat16)
    pert_out = (w_out + perturb_coef * grad_out).astype(jnp.bfloat16)
    second_in, second_out, second_sq = grad_sums(x_blocks, y_blocks, pert_in, pert_out)
    new_in = w_in - LEARN_RATE * (second_in * TOK_SCALE)
    new_out = w_out - LEARN_RATE * (second_out * TOK_SCALE)
    pert_loss = 0.5 * (second_sq * TOK_SCALE)
    return new_in, new_out, pert_loss
```

```python
import functools
import math

import jax
import jax.numpy as jnp
from jax import lax
from jax.experimental import pallas as pl
from jax.experimental.pallas import tpu as pltpu
from jax.sharding import PartitionSpec as P

RHO_FRAC = 0.1
LEARN_RATE = 1.0
N_TILES = 4
GELU_C0 = math.sqrt(2.0 / math.pi)
GELU_C1 = GELU_C0 * 0.044715
BF = jnp.bfloat16
F32 = jnp.float32
MESH = pl.DeviceIdType.MESH
ANY = pl.ANY
VMEM_BYTES = 67043328
D2D, P1, P2, G2, G1, GD = range(6)


def dot(left, right, left_dim, right_dim):
    return lax.dot_general(left, right, (((left_dim,), (right_dim,)), ((), ())), preferred_element_type=F32)


def gelu(z):
    th = jnp.tanh(z * (z * z * GELU_C1 + GELU_C0))
    half = 0.5 * z
    return half * th + half


def gelu_and_slope(z):
    sq = z * z
    th = jnp.tanh(z * (sq * GELU_C1 + GELU_C0))
    half = 0.5 * z
    up = th + 1.0
    bend = (half * (1.0 - th)) * (sq * (3.0 * GELU_C1) + GELU_C0)
    return half * up, up * (bend + 0.5)


def place():
    me = lax.axis_index("data")
    core, cx, cy = lax.rem(me, 2), lax.rem(me // 2, 2), me // 4
    return me, core, cx, cy, me + 1 - 2 * core, me + 2 - 4 * cx, me + 4 - 8 * cy


def greet(peers):
    barrier = pltpu.get_barrier_semaphore()
    for peer in peers:
        pl.semaphore_signal(barrier, inc=1, device_id=(peer,), device_id_type=MESH)
    pl.semaphore_wait(barrier, len(peers))


def remote(src, dst, send_sem, recv_sem, peer):
    return pltpu.make_async_remote_copy(src_ref=src, dst_ref=dst, send_sem=send_sem, recv_sem=recv_sem,
                                        device_id=(peer,), device_id_type=MESH)


def share_copies(me, gath, send, recv):
    return [remote(gath.at[me], gath.at[me], send.at[k], recv.at[k], lax.rem(me + k + 1, 8)) for k in range(7)]


def fold_rows(err, d_model):
    sq = err * err
    part = jnp.sum(sq.reshape(sq.shape[0] // 8, 8, d_model), axis=0)
    return part[:, :128] + part[:, 128:256] + part[:, 256:]


def forward_tile(rows, wi, wo, z_ref, h_ref, err_ref, loss_ref, y_ref, h_all, a_s, last):
    h = h_all[rows, :]
    h_ref[0] = h
    z = dot(h, wi, 1, 0).astype(BF)
    z_ref[0] = z
    a_s[...] = gelu(z.astype(F32)).astype(BF)
    u = dot(a_s[...], wo, 1, 0)
    h_next = (h.astype(F32) + u).astype(BF)
    h_all[rows, :] = h_next

    @pl.when(last)
    def _():
        err = h_next.astype(F32) - y_ref[...].astype(F32)
        err_ref[rows, :] = err.astype(BF)
        loss_ref[...] += fold_rows(err, err.shape[1])


def forward_kernel(x_ref, y_ref, wi_ref, wo_ref, z_ref, h_ref, err_ref, loss_ref, vi_ref, vo_ref, h_all, a_s):
    layer, tile = pl.program_id(0), pl.program_id(1)
    rows = pl.ds(tile * a_s.shape[0], a_s.shape[0])

    @pl.when(layer == 0)
    def _():
        h_all[rows, :] = x_ref[...]

    @pl.when((layer == 0) & (tile == 0))
    def _():
        loss_ref[...] = jnp.zeros_like(loss_ref)

    @pl.when(tile == 0)
    def _():
        vi_ref[0] = wi_ref[0].astype(BF)
        vo_ref[0] = wo_ref[0].astype(BF)

    forward_tile(rows, vi_ref[0], vo_ref[0], z_ref, h_ref, err_ref, loss_ref, y_ref, h_all, a_s,
                 layer == pl.num_programs(0) - 1)


def gather_kernel(n_layers, rho, x_ref, y_ref, sq_ref, g_hbm, wi_hbm, wo_hbm, z_ref, h_ref, err_ref, loss_ref, vi_ref, vo_ref,
                  h_all, a_s, v_buf, g_own, w_own, gath, load_sem, share_send, share_recv, send, recv):
    layer, tile = pl.program_id(0), pl.program_id(1)
    me, core, cx, cy, mate, nx, ny = place()
    d = g_own.shape[-1]
    half = d // 2
    rows = pl.ds(tile * a_s.shape[0], a_s.shape[0])
    row_a = pl.multiple_of(half * cy, half)
    row_b = pl.multiple_of(half * cx, half)

    def at_a(k):
        return v_buf.at[k, core, cx, pl.ds(row_a, half), :]

    def at_b(k):
        return v_buf.at[k, core, 2 + cy, pl.ds(row_b, half), :]

    def copies(stage, k):
        def one(ref, link, peer):
            return remote(ref, ref, send.at[stage - G2, link, k], recv.at[stage - G2, link, k], peer)

        if stage == G2:
            return [one(at_a(k), 0, ny), one(at_b(k), 1, nx)]
        if stage == G1:
            return [one(v_buf.at[k, core, cx], 0, nx), one(v_buf.at[k, core, 2 + cy], 1, ny)]
        return [one(v_buf.at[k, core], 0, mate)]

    def start(stage, k):
        for copy in copies(stage, k):
            copy.start()

    def wait(stage, k):
        for copy in copies(stage, k):
            copy.wait()

    @pl.when((layer == 0) & (tile == 0))
    def _():
        loss_ref[...] = jnp.zeros_like(loss_ref)
        load_g = pltpu.make_async_copy(g_hbm, g_own, load_sem.at[0])
        load_g.start()

        @pl.when(core == 0)
        def _():
            for k in range(n_layers):
                pltpu.make_async_copy(wi_hbm.at[k, pl.ds(row_a, half), pl.ds(pl.multiple_of(d * cx, d), d)],
                                      w_own.at[k, 0], load_sem.at[1]).start()
                pltpu.make_async_copy(wi_hbm.at[k, pl.ds(row_b, half), pl.ds(pl.multiple_of(d * (2 + cy), d), d)],
                                      w_own.at[k, 1], load_sem.at[1]).start()

        @pl.when(core == 1)
        def _():
            for k in range(n_layers):
                pltpu.make_async_copy(wo_hbm.at[k, pl.ds(pl.multiple_of(d * cx + row_a, half), half), :],
                                      w_own.at[k, 0], load_sem.at[1]).start()
                pltpu.make_async_copy(wo_hbm.at[k, pl.ds(pl.multiple_of(d * (2 + cy) + row_b, half), half), :],
                                      w_own.at[k, 1], load_sem.at[1]).start()

        greet([lax.rem(me + k + 1, 8) for k in range(7)])
        gath[me] = sq_ref[...]
        shares = share_copies(me, gath, share_send, share_recv)
        for copy in shares:
            copy.start()
        load_g.wait()
        pltpu.make_async_copy(g_hbm, w_own, load_sem.at[1]).wait()
        for copy in shares:
            copy.wait()
        total = jnp.sum(gath[...])
        coef = rho / jnp.sqrt(jnp.full((1, d), total, F32))

        def perturb(k, carry):
            at_a(k)[...] = (w_own[k, 0] + coef * g_own[k, 0]).astype(BF)
            at_b(k)[...] = (w_own[k, 1] + coef * g_own[k, 1]).astype(BF)
            return carry

        lax.fori_loop(0, n_layers, perturb, 0)
        start(G2, 0)
        start(G2, 1)
        wait(G2, 0)
        start(G1, 0)
        wait(G2, 1)
        start(G2, 2)
        wait(G1, 0)
        start(GD, 0)
        start(G1, 1)

    @pl.when(tile == 0)
    def _():
        @pl.when(layer + 1 < n_layers)
        def _():
            wait(G1, layer + 1)

        wait(GD, layer)

        @pl.when(layer + 1 < n_layers)
        def _():
            start(GD, layer + 1)

        @pl.when(layer + 2 < n_layers)
        def _():
            wait(G2, layer + 2)
            start(G1, layer + 2)

        @pl.when(layer + 3 < n_layers)
        def _():
            start(G2, layer + 3)

        for blk in range(4):
            vi_ref[0, :, blk * d:(blk + 1) * d] = v_buf[layer, 0, blk]
            vo_ref[0, blk * d:(blk + 1) * d, :] = v_buf[layer, 1, blk]

    @pl.when(layer == 0)
    def _():
        h_all[rows, :] = x_ref[...]

    forward_tile(rows, vi_ref[0], vo_ref[0], z_ref, h_ref, err_ref, loss_ref, y_ref, h_all, a_s, layer == n_layers - 1)


def backward_kernel(full, n_layers, scale, *refs):
    n_in = 8 if full else 5
    n_out = 3 if full else 2
    ins, outs, scr = refs[:n_in], refs[n_in:n_in + n_out], list(refs[n_in + n_out:])
    q_ref, z_ref, h_ref, vi_ref, vo_ref = ins[:5]
    q_s, acc_i, acc_o, a_s, p_s, s_buf, rd, rp1, rp2, send, recv, q_sem = scr[:12]
    step, tile = pl.program_id(0), pl.program_id(1)
    me, core, cx, cy, mate, nx, ny = place()
    d = rd.shape[-1]
    half = d // 2
    tok = a_s.shape[0]
    keep_a = pl.ds(pl.multiple_of(half * cy, half), half)
    give_a = pl.ds(pl.multiple_of(half * (1 - cy), half), half)
    keep_b = pl.ds(pl.multiple_of(half * cx, half), half)
    give_b = pl.ds(pl.multiple_of(half * (1 - cx), half), half)
    if full:
        loss_ref, wi_hbm, wo_hbm = ins[5:]
        wi_new, wo_new, loss_out = outs
        tot, w_i, w_o, gath, share_send, share_recv, load_sem, store_sem = scr[12:]
    else:
        g_out, sq_out = outs
        own, own_sem = scr[12:]

    def copies(stage, k):
        par, par3 = lax.rem(k, 2), lax.rem(k, 3)

        def one(src, dst, link, peer):
            return remote(src, dst, send.at[stage, link, par], recv.at[stage, link, par], peer)

        if stage == D2D:
            return [one(s_buf.at[1 - core], rd.at[par3], 0, mate)]
        if stage == P1:
            return [one(rd.at[par3, 1 - cx], rp1.at[par, 0], 0, nx), one(rd.at[par3, 3 - cy], rp1.at[par, 1], 1, ny)]
        if stage == P2:
            return [one(rd.at[par3, cx, give_a, :], rp2.at[par, 0], 0, ny),
                    one(rd.at[par3, 2 + cy, give_b, :], rp2.at[par, 1], 1, nx)]
        if stage == G2:
            part_a, part_b = tot.at[par3, core, cx, keep_a, :], tot.at[par3, core, 2 + cy, keep_b, :]
            return [one(part_a, part_a, 0, ny), one(part_b, part_b, 1, nx)]
        if stage == G1:
            part_a, part_b = tot.at[par3, core, cx], tot.at[par3, core, 2 + cy]
            return [one(part_a, part_a, 0, nx), one(part_b, part_b, 1, ny)]
        whole = tot.at[par3, core]
        return [one(whole, whole, 0, mate)]

    def start(stage, k):
        for copy in copies(stage, k):
            copy.start()

    def wait(stage, k):
        for copy in copies(stage, k):
            copy.wait()

    def when_layer(lag, body):
        @pl.when((step >= lag) & (step - lag < n_layers))
        def _():
            body(step - lag)

    def finish_pair(k):
        wait(D2D, k)
        par3 = lax.rem(k, 3)
        for blk in range(4):
            rd[par3, blk] += s_buf[core, blk]
        start(P1, k)

    def finish_p1(k):
        wait(P1, k)
        par, par3 = lax.rem(k, 2), lax.rem(k, 3)
        rd[par3, cx] += rp1[par, 0]
        rd[par3, 2 + cy] += rp1[par, 1]
        start(P2, k)

    def owned(k):
        wait(P2, k)
        par, par3 = lax.rem(k, 2), lax.rem(k, 3)
        return (rd[par3, cx, keep_a, :] + rp2[par, 0]) * scale, (rd[par3, 2 + cy, keep_b, :] + rp2[par, 1]) * scale

    @pl.when((step == 0) & (tile == 0))
    def _():
        pltpu.make_async_copy(q_ref, q_s, q_sem.at[0]).start()
        if full:
            pltpu.make_async_copy(wi_hbm.at[n_layers - 1], w_i, load_sem.at[0]).start()
            pltpu.make_async_copy(wo_hbm.at[n_layers - 1], w_o, load_sem.at[1]).start()
            greet([lax.rem(me + k + 1, 8) for k in range(7)])
            gath[me] = loss_ref[...]
            for copy in share_copies(me, gath, share_send, share_recv):
                copy.start()
        else:
            greet([mate, nx, ny])
            sq_out[...] = jnp.zeros_like(sq_out)
        pltpu.make_async_copy(q_ref, q_s, q_sem.at[0]).wait()

    if full:
        @pl.when((step == 1) & (tile == 0))
        def _():
            for copy in share_copies(me, gath, share_send, share_recv):
                copy.wait()
            loss_out[...] = jnp.full(loss_out.shape, 0.5 * (jnp.sum(gath[...]) * scale), F32)

    def start_pair(k):
        start(D2D, k)

    @pl.when(tile == 0)
    def _():
        when_layer(1, start_pair)
        if not full:
            when_layer(2, finish_p1)
        else:
            def keep_own(k):
                part_a, part_b = owned(k)
                par3 = lax.rem(k, 3)
                tot[par3, core, cx, keep_a, :] = part_a
                tot[par3, core, 2 + cy, keep_b, :] = part_b

            when_layer(2, keep_own)
            when_layer(1, finish_pair)

            def update_in(k):
                wait(GD, k)
                par3 = lax.rem(k, 3)
                pltpu.make_async_copy(wi_hbm.at[n_layers - 1 - k], w_i, load_sem.at[0]).wait()
                for blk in range(4):
                    cols = slice(blk * d, (blk + 1) * d)
                    w_i[:, cols] = w_i[:, cols] - LEARN_RATE * tot[par3, 0, blk]
                pltpu.make_async_copy(w_i, wi_new.at[n_layers - 1 - k], store_sem.at[0]).start()

            when_layer(4, update_in)

    @pl.when(tile == 1)
    def _():
        if not full:
            when_layer(1, finish_pair)
        else:
            def pass_on(k):
                wait(G2, k)
                start(G1, k)

            when_layer(3, pass_on)

            def update_out(k):
                par3 = lax.rem(k, 3)
                pltpu.make_async_copy(wo_hbm.at[n_layers - 1 - k], w_o, load_sem.at[1]).wait()
                for blk in range(4):
                    cols = slice(blk * d, (blk + 1) * d)
                    w_o[cols, :] = w_o[cols, :] - LEARN_RATE * tot[par3, 1, blk]
                pltpu.make_async_copy(w_o, wo_new.at[n_layers - 1 - k], store_sem.at[1]).start()

            when_layer(4, update_out)

    @pl.when(tile == 2)
    def _():
        if not full:
            def hand_out(k):
                par = lax.rem(k, 2)

                @pl.when(k >= 2)
                def _():
                    pltpu.make_async_copy(own.at[par], g_out.at[n_layers - 1 - k], own_sem.at[par]).wait()

                for j, part in enumerate(owned(k)):
                    own[par, j] = part
                    sq_out[...] += fold_rows(part, d)
                pltpu.make_async_copy(own.at[par], g_out.at[n_layers - 1 - k], own_sem.at[par]).start()

                @pl.when(k == n_layers - 1)
                def _():
                    pltpu.make_async_copy(own.at[1 - par], g_out.at[n_layers - 1 - k], own_sem.at[1 - par]).wait()
                    pltpu.make_async_copy(own.at[par], g_out.at[n_layers - 1 - k], own_sem.at[par]).wait()

            when_layer(2, hand_out)
        else:
            when_layer(1, finish_p1)

            def reload_in(k):
                pltpu.make_async_copy(w_i, wi_new.at[n_layers - 1 - k], store_sem.at[0]).wait()

                @pl.when(k < n_layers - 1)
                def _():
                    pltpu.make_async_copy(wi_hbm.at[n_layers - 2 - k], w_i, load_sem.at[0]).start()

            when_layer(4, reload_in)

    if full:
        @pl.when(tile == 3)
        def _():
            def cross(k):
                wait(G1, k)
                start(GD, k)

            when_layer(3, cross)
            when_layer(2, functools.partial(start, G2))

            def reload_out(k):
                pltpu.make_async_copy(w_o, wo_new.at[n_layers - 1 - k], store_sem.at[1]).wait()

                @pl.when(k < n_layers - 1)
                def _():
                    pltpu.make_async_copy(wo_hbm.at[n_layers - 2 - k], w_o, load_sem.at[1]).start()

            when_layer(4, reload_out)

    @pl.when(step < n_layers)
    def _():
        rows = pl.ds(tile * tok, tok)

        @pl.when(tile == 0)
        def _():
            acc_i[...] = jnp.zeros_like(acc_i)
            acc_o[...] = jnp.zeros_like(acc_o)

        q = q_s[rows, :]
        da = dot(q, vo_ref[0], 1, 1)
        act, slope = gelu_and_slope(z_ref[0].astype(F32))
        a_s[...] = act.astype(BF)
        p_s[...] = (da * slope).astype(BF)
        acc_i[...] += dot(h_ref[0], p_s[...], 0, 0)
        acc_o[...] += dot(q, a_s[...], 0, 0)
        back = dot(p_s[...], vi_ref[0], 1, 1)
        q_s[rows, :] = (q.astype(F32) + back).astype(BF)

        @pl.when(tile == N_TILES - 1)
        def _():
            for blk in range(4):
                cols = slice(blk * d, (blk + 1) * d)
                s_buf[0, blk] = acc_i[:, cols]
                s_buf[1, blk] = acc_o[:, cols].T


def solution(mesh):
    n_dev = mesh.shape["data"]

    def local_step(x_loc, y_loc, w_in, w_out):
        n_layers, d, ff = w_in.shape
        tokens = x_loc.shape[0] * x_loc.shape[1]
        tok = tokens // N_TILES
        scale = 1.0 / (tokens * n_dev * d)
        rho = RHO_FRAC * math.sqrt(n_layers * (d + ff))
        x_flat, y_flat = x_loc.reshape(tokens, d), y_loc.reshape(tokens, d)
        shape = jax.ShapeDtypeStruct
        dma, vmem = pltpu.SemaphoreType.DMA, pltpu.VMEM
        last = n_layers - 1
        tile_x = pl.BlockSpec((tok, d), lambda l, t: (jnp.where(l == 0, t, N_TILES - 1), 0))
        tile_y = pl.BlockSpec((tok, d), lambda l, t: (jnp.where(l == last, t, 0), 0))
        small = pl.BlockSpec((8, 128), lambda l, t: (0, 0))
        hbm = pl.BlockSpec(memory_space=ANY)

        def layer_of(rows, cols):
            return pl.BlockSpec((1, rows, cols), lambda l, t: (l, 0, 0))

        act_specs = [pl.BlockSpec((1, tok, ff), lambda l, t: (l, t, 0)), pl.BlockSpec((1, tok, d), lambda l, t: (l, t, 0)),
                     pl.BlockSpec((tokens, d), lambda l, t: (0, 0)), small, layer_of(d, ff), layer_of(ff, d)]
        act_shapes = [shape((n_layers, tokens, ff), BF), shape((n_layers, tokens, d), BF), shape((tokens, d), BF),
                      shape((8, 128), F32), shape((n_layers, d, ff), BF), shape((n_layers, ff, d), BF)]
        mul = 2 * tokens * d * ff * n_layers

        z_1, h_1, q_1, _, vi_1, vo_1 = pl.pallas_call(
            forward_kernel, name="forward", grid=(n_layers, N_TILES),
            in_specs=[tile_x, tile_y, layer_of(d, ff), layer_of(ff, d)],
            out_specs=act_specs, out_shape=act_shapes,
            scratch_shapes=[vmem((tokens, d), BF), vmem((tok, ff), BF)],
            cost_estimate=pl.CostEstimate(flops=2 * mul, bytes_accessed=10 ** 8, transcendentals=0),
            compiler_params=pltpu.CompilerParams(vmem_limit_bytes=VMEM_BYTES),
        )(x_flat, y_flat, w_in, w_out)

        def backward(full, q_0, z_all, h_all, vi, vo, *extra):
            n_steps = n_layers + (4 if full else 2)

            def at_layer(*block):
                def index(l, t):
                    live = l < n_layers
                    row = jnp.where(live, t, N_TILES - 1) if block[0] == tok else 0
                    return (jnp.maximum(last - l, 0), row, 0)
                return pl.BlockSpec((1,) + block, index)

            in_specs = [hbm, at_layer(tok, ff), at_layer(tok, d),
                        at_layer(d, ff), at_layer(ff, d)]
            scratch = [vmem((tokens, d), BF), vmem((d, ff), F32), vmem((d, ff), F32), vmem((tok, ff), BF), vmem((tok, ff), BF),
                       vmem((2, 4, d, d), F32), vmem((3, 4, d, d), F32), vmem((2, 2, d, d), F32), vmem((2, 2, d // 2, d), F32),
                       dma((6 if full else 3, 2, 2)), dma((6 if full else 3, 2, 2)), dma((1,))]
            if full:
                in_specs += [small, hbm, hbm]
                out_specs = [hbm, hbm, small]
                out_shape = [shape((n_layers, d, ff), F32), shape((n_layers, ff, d), F32), shape((8, 128), F32)]
                scratch += [vmem((3, 2, 4, d, d), F32), vmem((d, ff), F32), vmem((ff, d), F32), vmem((8, 8, 128), F32),
                            dma((7,)), dma((7,)), dma((2,)), dma((2,))]
            else:
                out_specs = [hbm, small]
                out_shape = [shape((n_layers, 2, d // 2, d), F32), shape((8, 128), F32)]
                scratch += [vmem((2, 2, d // 2, d), F32), dma((2,))]
            return pl.pallas_call(
                functools.partial(backward_kernel, full, n_layers, scale), name="backward_full" if full else "backward",
                grid=(n_steps, N_TILES), in_specs=in_specs, out_specs=out_specs, out_shape=out_shape, scratch_shapes=scratch,
                cost_estimate=pl.CostEstimate(flops=4 * mul, bytes_accessed=3 * 10 ** 8, transcendentals=0),
                compiler_params=pltpu.CompilerParams(vmem_limit_bytes=VMEM_BYTES, collective_id=2 if full else 0,
                                                     has_side_effects=True),
            )(q_0, z_all, h_all, vi, vo, *extra)

        g_own, sq_own = backward(False, q_1, z_1, h_1, vi_1, vo_1)

        z_2, h_2, q_2, loss_2, vi_2, vo_2 = pl.pallas_call(
            functools.partial(gather_kernel, n_layers, rho), name="gather_forward", grid=(n_layers, N_TILES),
            in_specs=[tile_x, tile_y, small, hbm, hbm, hbm],
            out_specs=act_specs, out_shape=act_shapes,
            scratch_shapes=[vmem((tokens, d), BF), vmem((tok, ff), BF), vmem((n_layers, 2, 4, d, d), BF),
                            vmem((n_layers, 2, d // 2, d), F32), vmem((n_layers, 2, d // 2, d), F32), vmem((8, 8, 128), F32),
                            dma((2,)), dma((7,)), dma((7,)), dma((3, 2, n_layers)), dma((3, 2, n_layers))],
            cost_estimate=pl.CostEstimate(flops=2 * mul, bytes_accessed=10 ** 8, transcendentals=0),
            compiler_params=pltpu.CompilerParams(vmem_limit_bytes=VMEM_BYTES, collective_id=1, has_side_effects=True),
        )(x_flat, y_flat, sq_own, g_own, w_in, w_out)

        new_in, new_out, loss = backward(True, q_2, z_2, h_2, vi_2, vo_2, loss_2, w_in, w_out)
        return new_in, new_out, loss[0, 0]

    return jax.shard_map(local_step, mesh=mesh, in_specs=(P("data"), P("data"), P(), P()), out_specs=(P(), P(), P()), check_vma=False)
```
